32 devices in a mesh: ga: 8 (over y, x, core), ba: 4 (over z).
Axes of the slice: x: 2, y: 2, z: 4, core: 2. Of those that a mesh axis runs over, the one named last changes fastest.
Arguments:
- psi: float32 [2, 16384, 2048], P(None, 'ga', 'ba'), may hold values from -0.1875 to 0.1875
- dpsi: float32 [2, 16384, 512], P(None, 'ga', 'ba'), may hold values from -6 to 6
- band_weight: float32 [2048], replicated, may hold values from 0.25 to 1
- panel_band: int32 [16], P('ba'), may hold values from 0 to 15, each once
- slab_offset: int32 [8], replicated, may hold values from 0 to 2047
Outputs:
- projected: float32 [2, 16384, 512], P(None, 'ga', 'ba')
The draws below stay inside these ranges and needn't reach their ends.
Inputs may be any that keep to these rules, and one draw needn't show every extreme that they name: panel_band is a permutation of the panel numbers.
All inputs are finite; a program needn't handle non-finite values.
Results may differ from the reference program's by a relative error of at most 0.00012.
Values sent between devices are 32-bit elements; how exact they have to be, the bound alone decides.
A program may use at most 128 MiB of HBM per device.

```python
import math
import jax
import jax.numpy as jnp
from jax import lax

NB = 2048
NP = 512
PANEL = 128
NPW_DEV = 2048
NPW = 16384
NPANEL = 16
N_GA = 8


def place_ends(array, rng, low, high):
    place = [jax.random.randint(jax.random.fold_in(rng, axis), (), 0, length) for axis, length in enumerate(array.shape)]
    widest = array.shape.index(max(array.shape))
    neighbour = place[:widest] + [(place[widest] + 1) % array.shape[widest]] + place[widest + 1:]
    return array.at[tuple(place)].set(low).at[tuple(neighbour)].set(high)


def block_scale(rng, shape, shards, least, top_value):
    def one(position, shards_of):
        steps = jax.random.uniform(jax.random.fold_in(jax.random.fold_in(rng, 6), position), (shards_of,), jnp.float32, least / len(shards), top_value / len(shards))
        return jnp.repeat(jnp.exp(steps), shape[position] // shards_of).reshape((-1,) + (1,) * (len(shape) - position - 1))

    factor_of = one(*shards[0])
    for cut in shards[1:]:
        factor_of = factor_of * one(*cut)
    return factor_of


def scatter_about(key, extent, deviation, reach, shards=(), held_as=jnp.bfloat16):
    drawn = jax.random.normal(key, extent, jnp.float32) * deviation
    if len(shards) > 0:
        drawn = block_scale(key, extent, shards, -0.22, 0.18) * drawn
    return jnp.clip(drawn, min=-reach, max=reach).astype(held_as)


def setup_inputs(seed: int = 0) -> dict:
    seeds = jax.random.split(jax.random.key(seed), 6)
    return {
        "psi": scatter_about(seeds[0], (2, NPW, NB), ((NPW * NB) ** -0.25), 0.1875, ((1, 8), (2, 4)), jnp.float32),
        "dpsi": scatter_about(seeds[1], (2, NPW, NP), 1.0, 6.0, ((1, 8), (2, 4)), jnp.float32),
        "band_weight": jnp.clip(jnp.exp(jax.random.uniform(seeds[2], (NB,), jnp.float32, math.log(0.25), math.log(1.0))), 0.25, 1.0),
        "panel_band": jax.random.permutation(seeds[3], NPANEL).astype(jnp.int32),
        "slab_offset": place_ends(jax.random.randint(seeds[4], (N_GA,), 0, NPW_DEV), jax.random.fold_in(seeds[4], 1), 0, NPW_DEV - 1).astype(jnp.int32),
    }


def tdot(left, right):
    return lax.dot_general(left, right, (((0,), (0,)), ((), ())), precision=lax.Precision.HIGHEST, preferred_element_type=jnp.float32)


def mdot(left, right):
    return jnp.dot(left, right, precision=lax.Precision.HIGHEST, preferred_element_type=jnp.float32)


def reference(psi, dpsi, band_weight, panel_band, slab_offset):
    stacked = dpsi.reshape(2, N_GA, NPW_DEV, NP)
    rows = (jnp.arange(NPW_DEV, dtype=jnp.int32)[None, :] + slab_offset[:, None]) % NPW_DEV
    aligned = jnp.take_along_axis(stacked, rows[None, :, :, None], axis=2).reshape(2, NPW, NP)
    weight = band_weight.reshape(NPANEL, PANEL)[panel_band].reshape(NB)
    over_re = tdot(psi[0], aligned[0]) + tdot(psi[1], aligned[1])
    over_im = tdot(psi[0], aligned[1]) - tdot(psi[1], aligned[0])
    w_re = over_re * weight[:, None]
    w_im = over_im * weight[:, None]
    corr_re = mdot(psi[0], w_re) - mdot(psi[1], w_im)
    corr_im = mdot(psi[0], w_im) + mdot(psi[1], w_re)
    diff = (aligned - jnp.stack([corr_re, corr_im])).reshape(2, N_GA, NPW_DEV, NP)
    back = (jnp.arange(NPW_DEV, dtype=jnp.int32)[None, :] - slab_offset[:, None]) % NPW_DEV
    result = jnp.take_along_axis(diff, back[None, :, :, None], axis=2)
    return result.reshape(2, NPW, NP)
```

```python
import functools

import jax
import jax.numpy as jnp
from jax import lax
from jax.sharding import PartitionSpec as P

PANEL = 128


def tdot(left, right):
    return lax.dot_general(
        left,
        right,
        (((0,), (0,)), ((), ())),
        precision=lax.Precision.HIGH,
        preferred_element_type=jnp.float32,
    )


def mdot(left, right):
    return jnp.dot(left, right, precision=lax.Precision.HIGH, preferred_element_type=jnp.float32)


CHUNKS = 2


def turned(packed, width):
    column = lax.broadcasted_iota(jnp.int32, packed.shape, 1)
    first = (column // width) % 2 == 0
    return jnp.where(first, jnp.roll(packed, -width, axis=1), -jnp.roll(packed, width, axis=1))


def sum_over(block, axis, size):
    if size & (size - 1) or block.shape[0] % size:
        return lax.psum(block, axis)
    place = lax.axis_index(axis)
    bits = [1 << b for b in range(size.bit_length() - 1)]
    for bit in bits:
        upper = (place // bit) % 2
        half = block.shape[0] // 2
        kept = lax.dynamic_slice_in_dim(block, upper * half, half, 0)
        sent = lax.dynamic_slice_in_dim(block, (1 - upper) * half, half, 0)
        block = kept + lax.ppermute(sent, axis, [(i, i ^ bit) for i in range(size)])
    for bit in reversed(bits):
        upper = (place // bit) % 2 == 1
        other = lax.ppermute(block, axis, [(i, i ^ bit) for i in range(size)])
        block = jnp.concatenate([jnp.where(upper, other, block), jnp.where(upper, block, other)])
    return block


def weights_for(band_weight, panels):
    table = band_weight.reshape(-1, PANEL)
    onehot = (panels[:, None] == jnp.arange(table.shape[0], dtype=jnp.int32)[None, :]).astype(
        jnp.float32
    )
    return mdot(onehot, table).reshape(-1)


def per_device(size, psi, dpsi, band_weight, panel_band, slab_offset):
    offset = slab_offset[lax.axis_index("ga")]
    aligned = jnp.roll(dpsi, -offset, axis=1)
    local_weight = weights_for(band_weight, panel_band)
    width = aligned.shape[2] // CHUNKS
    pieces = []
    for chunk in range(CHUNKS):
        columns = slice(chunk * width, (chunk + 1) * width)
        own = jnp.concatenate([aligned[0, :, columns], aligned[1, :, columns]], axis=1)
        every = lax.all_gather(own, "ba", axis=1, tiled=True)
        block = tdot(psi[0], every) + turned(tdot(psi[1], every), width)
        weighted = sum_over(block, "ga", size) * local_weight[:, None]
        correction = mdot(psi[0], weighted) - mdot(psi[1], turned(weighted, width))
        share = lax.psum_scatter(correction, "ba", scatter_dimension=1, tiled=True)
        pieces.append(own - share)
    result = jnp.stack(
        [
            jnp.concatenate([piece[:, part * width : (part + 1) * width] for piece in pieces], axis=1)
            for part in range(2)
        ]
    )
    return jnp.roll(result, offset, axis=1)


def solution(mesh):
    in_specs = (P(None, "ga", "ba"), P(None, "ga", "ba"), P(), P("ba"), P())
    out_specs = P(None, "ga", "ba")
    return jax.shard_map(
        functools.partial(per_device, mesh.shape["ga"]), mesh=mesh, in_specs=in_specs, out_specs=out_specs, check_vma=False
    )
```

```python
import functools

import jax
import jax.numpy as jnp
from jax import lax
from jax.sharding import PartitionSpec as P

PANEL = 128


def tdot(left, right):
    return lax.dot_general(
        left,
        right,
        (((0,), (0,)), ((), ())),
        precision=lax.Precision.HIGH,
        preferred_element_type=jnp.float32,
    )


def mdot(left, right):
    return jnp.dot(left, right, precision=lax.Precision.HIGH, preferred_element_type=jnp.float32)


CHUNKS = 2


def turned(packed, width):
    column = lax.broadcasted_iota(jnp.int32, packed.shape, 1)
    first = (column // width) % 2 == 0
    return jnp.where(first, jnp.roll(packed, -width, axis=1), -jnp.roll(packed, width, axis=1))


def sum_over(block, axis, size):
    if size & (size - 1) or block.shape[0] % size:
        return lax.psum(block, axis)
    place = lax.axis_index(axis)
    bits = [1 << b for b in range(size.bit_length() - 1)]
    for bit in bits:
        upper = (place // bit) % 2
        half = block.shape[0] // 2
        kept = lax.dynamic_slice_in_dim(block, upper * half, half, 0)
        sent = lax.dynamic_slice_in_dim(block, (1 - upper) * half, half, 0)
        block = kept + lax.ppermute(sent, axis, [(i, i ^ bit) for i in range(size)])
    for bit in reversed(bits):
        upper = (place // bit) % 2 == 1
        other = lax.ppermute(block, axis, [(i, i ^ bit) for i in range(size)])
        block = jnp.concatenate([jnp.where(upper, other, block), jnp.where(upper, block, other)])
    return block


def weights_for(band_weight, panels):
    table = band_weight.reshape(-1, PANEL)
    onehot = (panels[:, None] == jnp.arange(table.shape[0], dtype=jnp.int32)[None, :]).astype(
        jnp.float32
    )
    return mdot(onehot, table).reshape(-1)


def per_device(size, psi, dpsi, band_weight, panel_band, slab_offset):
    offset = slab_offset[lax.axis_index("ga")]
    aligned = jnp.roll(dpsi, -offset, axis=1)
    local_weight = weights_for(band_weight, panel_band)
    width = aligned.shape[2] // CHUNKS
    owns, corrections = [], []
    for chunk in range(CHUNKS):
        columns = slice(chunk * width, (chunk + 1) * width)
        own = jnp.concatenate([aligned[0, :, columns], aligned[1, :, columns]], axis=1)
        every = lax.all_gather(own, "ba", axis=1, tiled=True)
        if corrections:
            every, corrections[-1] = lax.optimization_barrier((every, corrections[-1]))
        block = tdot(psi[0], every) + turned(tdot(psi[1], every), width)
        weighted = sum_over(block, "ga", size) * local_weight[:, None]
        owns.append(own)
        corrections.append(mdot(psi[0], weighted) - mdot(psi[1], turned(weighted, width)))
    pieces = [
        own - lax.psum_scatter(correction, "ba", scatter_dimension=1, tiled=True)
        for own, correction in zip(owns, corrections)
    ]
    result = jnp.stack(
        [
            jnp.concatenate([piece[:, part * width : (part + 1) * width] for piece in pieces], axis=1)
            for part in range(2)
        ]
    )
    return jnp.roll(result, offset, axis=1)


def solution(mesh):
    in_specs = (P(None, "ga", "ba"), P(None, "ga", "ba"), P(), P("ba"), P())
    out_specs = P(None, "ga", "ba")
    return jax.shard_map(
        functools.partial(per_device, mesh.shape["ga"]), mesh=mesh, in_specs=in_specs, out_specs=out_specs, check_vma=False
    )
```
